32 devices in a mesh: section: 4 (over x, core), expert: 2 (over y), dp: 4 (over z).
Axes of the slice: x: 2, y: 2, z: 4, core: 2. Of those that a mesh axis runs over, the one named last changes fastest.
Arguments:
- fwd_input: bfloat16 [4, 256, 2048], P('section', 'dp', 'expert'), may hold values from -6 to 6
- fresh_input: bfloat16 [1, 256, 2048], P(None, 'dp', 'expert'), may hold values from -6 to 6
- fwd_experts: int32 [4, 2, 256, 2], P('section', None, 'dp'), may hold values from 0 to 3, all different within a row; in each aligned block of 64 rows (0 to 63, 64 to 127, ..., all dimensions but the last counted through in order) at most 36 rows name the same one
- fwd_gates: float32 [4, 2, 256, 2], P('section', None, 'dp'), may hold values from 0.2 to 1
- bwd_saved: bfloat16 [4, 2, 256, 2048], P('section', None, 'dp', 'expert'), may hold values from -6 to 6
- bwd_experts: int32 [4, 2, 256, 2], P('section', None, 'dp'), may hold values from 0 to 3, all different within a row; in each aligned block of 64 rows (0 to 63, 64 to 127, ..., all dimensions but the last counted through in order) at most 36 rows name the same one
- bwd_gates: float32 [4, 2, 256, 2], P('section', None, 'dp'), may hold values from 0.2 to 1
- out_grad: bfloat16 [4, 256, 2048], P('section', 'dp', 'expert'), may hold values from -6 to 6
- fresh_grad: bfloat16 [1, 256, 2048], P(None, 'dp', 'expert'), may hold values from -6 to 6
- gate_proj: bfloat16 [4, 4, 7168, 2048], P('section', 'dp', 'expert'), may hold values from -0.125 to 0.125
- down_proj: bfloat16 [4, 4, 7168, 2048], P('section', 'dp', 'expert'), may hold values from -0.0625 to 0.0625
Outputs:
- fwd_output: bfloat16 [4, 2, 256, 2048], P('section', None, 'dp', 'expert')
- input_grad: bfloat16 [4, 2, 256, 2048], P('section', None, 'dp', 'expert')
- gate_grad: bfloat16 [4, 4, 7168, 2048], P('section', 'dp', 'expert')
- down_grad: bfloat16 [4, 4, 7168, 2048], P('section', 'dp', 'expert')
The draws below stay inside these ranges and needn't reach their ends.
Inputs may be any that keep to these rules, and one draw needn't show every extreme that they name: `fwd_experts`: each token names two different experts. In every aligned block of 64 tokens (one index of dp, one section and step) no expert is named more than 36 times, and in some blocks one expert is named exactly 36 times. `bwd_experts`: each token names two different experts. In every aligned block of 64 tokens (one index of dp, one section and step) no expert is named more than 36 times, and in some blocks one expert is named exactly 36 times.
All inputs are finite; a program needn't handle non-finite values.
Results may differ from the reference program's by a relative error of at most 0.0062.
Values may be sent and summed in bfloat16 or wider, within the bound.
A program may use at most 256 MiB of HBM per device.

```python
import math
import jax
import jax.numpy as jnp
import numpy as np
from jax import lax

D = 2048
FF = 7168
EXPERTS = 4
TOK_DEV = 64
TICKS = 2
CAP = 36
SECTIONS = 4
BLOCKS = 2
TOKENS = 256


def block_scale(own_key, dims, shards, smallest, high):
    gain, own = 1.0, jax.random.fold_in(own_key, 6)
    for dim, shards_of in shards:
        steps = jnp.exp(jax.random.uniform(jax.random.fold_in(own, dim), (shards_of,), jnp.float32, smallest / len(shards), high / len(shards)))
        gain = gain * jnp.repeat(steps, dims[dim] // shards_of).reshape([-1 if axis == dim else 1 for axis in range(len(dims))])
    return gain


def shared_out(rng, own, number, rows, amount, top, limit, lean):
    sequence = jax.random.permutation(rng, amount)
    packed, common = shares(amount, rows * top, limit, lean, True), shares(amount, rows * top, limit, lean, False)
    places = jnp.arange(amount)

    def named(sizes, turn):
        used = int((sizes > 0).sum())
        fixed = max(1, used // 4)
        passed = fixed + (places - fixed + turn * (used - fixed)) % max(1, amount - fixed)
        return jnp.zeros((amount,), jnp.int32).at[sequence[jnp.where(places < fixed, places, passed)]].set(jnp.asarray(sizes, jnp.int32))

    sizes = jnp.where(number % 4 == 0, named(packed, number // 4), named(common, number - number // 4 - 1))
    mixed = jax.random.permutation(jax.random.fold_in(own, 3), amount)
    donor, receiver = mixed[0:amount // 2 * 2:2], mixed[1:amount // 2 * 2:2]
    room = jnp.minimum(sizes[donor] - 1, limit - sizes[receiver]) // 2
    room = jnp.where((donor == sequence[0]) | (receiver == sequence[0]) | (sizes[receiver] == 0), 0, jnp.maximum(room, 0))
    passed = jax.random.randint(jax.random.fold_in(own, 4), (amount // 2,), 0, 1 << 20) % (room + 1)
    sizes = sizes.at[donor].add(-passed).at[receiver].add(passed)
    members = jnp.searchsorted(jnp.cumsum(sizes), jnp.arange(rows * top), side="right").astype(jnp.int32)
    listing = members.reshape(top, rows).T
    listing = listing[jax.random.permutation(jax.random.fold_in(own, 1), rows)]
    turn = jax.random.randint(jax.random.fold_in(own, 2), (rows, 1), 0, top)
    return jnp.take_along_axis(listing, (jnp.arange(top)[None, :] + turn) % top, axis=1)


def shares(count, total, most, slope, full):
    weights = [(1 << 20) // math.isqrt(standing ** slope) + 1 for standing in range(1, count + 1)]
    largest = most if full else min(most, max(-(-total // count), total * weights[0] // sum(weights)))
    least = 1 if total - largest >= count - 1 else 0
    holding, surplus = [largest] + [least] * (count - 1), total - largest - least * (count - 1)
    while surplus > 0:
        free = [i for i in range(1, count) if holding[i] < largest] or [i for i in range(1, count) if holding[i] < most]
        mass, left = sum([weights[i] for i in free]), surplus
        for i in free:
            more = min(most - holding[i], max(1, left * weights[i] // mass), surplus)
            holding[i] = holding[i] + more
            surplus = surplus - more
    return np.array(holding)


def centred(key, shape, deviation, reach, cuts=(), held_as=jnp.bfloat16):
    drawn = deviation * jax.random.normal(key, shape, jnp.float32)
    if cuts:
        drawn = drawn * block_scale(key, shape, cuts, -0.22, 0.18)
    return jnp.clip(drawn, -reach, reach).astype(held_as)


def setup_inputs(seed: int = 0) -> dict:
    streams_of = jax.random.split(jax.random.key(seed), 12)
    fwd_input = centred(streams_of[0], (SECTIONS, TOKENS, D), 1.0, 6.0, ((0, 4), (1, 4), (2, 2)))
    fresh_input = centred(streams_of[1], (TICKS - 1, TOKENS, D), 1.0, 6.0, ((1, 4), (2, 2)))
    fwd_experts_keys = jax.random.split(jax.random.fold_in(streams_of[2], 1), SECTIONS * TICKS * TOKENS // TOK_DEV)
    fwd_experts_turns = jax.random.permutation(jax.random.fold_in(streams_of[2], 3), SECTIONS * TICKS * TOKENS // TOK_DEV)
    fwd_experts = jax.vmap(lambda own, number: shared_out(jax.random.fold_in(streams_of[2], 2), own, number, TOK_DEV, EXPERTS, 2, CAP, 2))(fwd_experts_keys, fwd_experts_turns).reshape((SECTIONS, TICKS, TOKENS, 2))
    fwd_gates = jnp.clip(0.2 + 0.8 * jax.random.uniform(streams_of[3], (SECTIONS, TICKS, TOKENS, 2), jnp.float32) ** block_scale(streams_of[3], (SECTIONS, TICKS, TOKENS, 2), ((0, 4), (2, 4)), -0.2, 0.2), 0.2, 1.0)
    bwd_saved = centred(streams_of[4], (SECTIONS, TICKS, TOKENS, D), 1.0, 6.0, ((0, 4), (2, 4), (3, 2)))
    bwd_experts_keys = jax.random.split(jax.random.fold_in(streams_of[5], 1), SECTIONS * TICKS * TOKENS // TOK_DEV)
    bwd_experts_turns = jax.random.permutation(jax.random.fold_in(streams_of[5], 3), SECTIONS * TICKS * TOKENS // TOK_DEV)
    bwd_experts = jax.vmap(lambda own, number: shared_out(jax.random.fold_in(streams_of[5], 2), own, number, TOK_DEV, EXPERTS, 2, CAP, 2))(bwd_experts_keys, bwd_experts_turns).reshape((SECTIONS, TICKS, TOKENS, 2))
    bwd_gates = jnp.clip(0.2 + 0.8 * jax.random.uniform(streams_of[6], (SECTIONS, TICKS, TOKENS, 2), jnp.float32) ** block_scale(streams_of[6], (SECTIONS, TICKS, TOKENS, 2), ((0, 4), (2, 4)), -0.2, 0.2), 0.2, 1.0)
    out_grad = centred(streams_of[7], (SECTIONS, TOKENS, D), 1.0, 6.0, ((0, 4), (1, 4), (2, 2)))
    fresh_grad = centred(streams_of[8], (TICKS - 1, TOKENS, D), 1.0, 6.0, ((1, 4), (2, 2)))
    gate_proj = centred(streams_of[9], (SECTIONS, EXPERTS, FF, D), D ** -0.5, 0.125, ((0, 4), (1, 4), (2, 2)))
    down_proj = centred(streams_of[10], (SECTIONS, EXPERTS, FF, D), FF ** -0.5, 0.0625, ((0, 4), (1, 4), (2, 2)))
    return dict(fwd_input=fwd_input, fresh_input=fresh_input, fwd_experts=fwd_experts, fwd_gates=fwd_gates, bwd_saved=bwd_saved, bwd_experts=bwd_experts, bwd_gates=bwd_gates, out_grad=out_grad, fresh_grad=fresh_grad, gate_proj=gate_proj, down_proj=down_proj)


precise = lax.Precision.HIGHEST

def block_sum(hidden, weight, blocks):
    length = hidden.shape[0]
    pieces = jnp.einsum('tbf,bfd->tbd', hidden.astype(jnp.float32).reshape(length, blocks, -1), weight.astype(jnp.float32).reshape(blocks, -1, weight.shape[-1]), precision=precise)
    rounded = lax.optimization_barrier(pieces.astype(jnp.bfloat16))
    return lax.optimization_barrier(jnp.sum(rounded.astype(jnp.float32), axis=1))

def routed_weight(experts, gate_values, number):
    return lax.optimization_barrier(jnp.sum(jnp.where(experts == number, gate_values, jnp.float32(0.0)), axis=1))

def layer_forward(inputs, experts, gate_values, gate_weight, down_weight):
    combined = inputs.astype(jnp.float32)
    for number in range(EXPERTS):
        weight_row = routed_weight(experts, gate_values, number)
        before_act = jnp.dot(inputs, gate_weight[number].T, preferred_element_type=jnp.float32)
        hidden = jax.nn.silu(before_act).astype(jnp.bfloat16)
        output = block_sum(hidden, down_weight[number], BLOCKS)
        combined = combined + weight_row[:, None] * output
    return combined.astype(jnp.bfloat16)

def layer_backward(stored, experts, gate_values, cotangent, gate_weight, down_weight):
    result = cotangent.astype(jnp.float32)
    gate_parts = []
    down_parts = []
    for number in range(EXPERTS):
        weight_row = routed_weight(experts, gate_values, number)
        scaled = (weight_row[:, None] * cotangent.astype(jnp.float32)).astype(jnp.bfloat16)
        before_act = jnp.dot(stored, gate_weight[number].T, preferred_element_type=jnp.float32)
        hidden = jax.nn.silu(before_act).astype(jnp.bfloat16)
        down_parts.append(jnp.dot(hidden.T, scaled, preferred_element_type=jnp.float32))
        through = jnp.dot(scaled, down_weight[number].T, preferred_element_type=jnp.float32)
        sigmoid = jax.nn.sigmoid(before_act)
        slope_grad = (through * sigmoid * (1.0 + before_act * (1.0 - sigmoid))).astype(jnp.bfloat16)
        gate_parts.append(jnp.dot(slope_grad.T, stored, preferred_element_type=jnp.float32))
        result = result + block_sum(slope_grad, gate_weight[number], BLOCKS)
    return (result.astype(jnp.bfloat16), jnp.stack(gate_parts), jnp.stack(down_parts))

def reference(fwd_input, fresh_input, fwd_experts, fwd_gates, bwd_saved, bwd_experts, bwd_gates, out_grad, fresh_grad, gate_proj, down_proj):
    forward = [[None for tick_index in range(TICKS)] for section_index in range(SECTIONS)]
    backward = [[None for tick_index in range(TICKS)] for section_index in range(SECTIONS)]
    gate_sums = [jnp.zeros((EXPERTS, FF, D), jnp.float32) for section_index in range(SECTIONS)]
    down_sums = [jnp.zeros((EXPERTS, FF, D), jnp.float32) for section_index in range(SECTIONS)]
    for tick_index in range(TICKS):
        for section_index in range(SECTIONS):
            if tick_index == 0:
                inputs = fwd_input[section_index]
            elif section_index == 0:
                inputs = fresh_input[tick_index - 1]
            else:
                inputs = forward[section_index - 1][tick_index - 1]
            forward[section_index][tick_index] = layer_forward(inputs, fwd_experts[section_index, tick_index], fwd_gates[section_index, tick_index], gate_proj[section_index], down_proj[section_index])
            if tick_index == 0:
                cotangent = out_grad[section_index]
            elif section_index == SECTIONS - 1:
                cotangent = fresh_grad[tick_index - 1]
            else:
                cotangent = backward[section_index + 1][tick_index - 1]
            result, gate_step, down_step = layer_backward(bwd_saved[section_index, tick_index], bwd_experts[section_index, tick_index], bwd_gates[section_index, tick_index], cotangent, gate_proj[section_index], down_proj[section_index])
            backward[section_index][tick_index] = result
            gate_sums[section_index] = gate_sums[section_index] + gate_step
            down_sums[section_index] = down_sums[section_index] + down_step
    squares = jnp.float32(0.0)
    for section_index in range(SECTIONS):
        squares = squares + jnp.sum(gate_sums[section_index] * gate_sums[section_index]) + jnp.sum(down_sums[section_index] * down_sums[section_index])
    clip_limit = 0.25 * math.sqrt(2.0 * SECTIONS * EXPERTS * FF * D)
    factor = clip_limit / jnp.maximum(jnp.sqrt(squares), clip_limit)
    fwd_output = jnp.stack([jnp.stack(forward[section_index]) for section_index in range(SECTIONS)])
    input_grad = jnp.stack([jnp.stack(backward[section_index]) for section_index in range(SECTIONS)])
    gate_grad = (jnp.stack(gate_sums) * factor).astype(jnp.bfloat16)
    down_grad = (jnp.stack(down_sums) * factor).astype(jnp.bfloat16)
    return (fwd_output, input_grad, gate_grad, down_grad)
```

```python
import functools
import math

import jax
import jax.numpy as jnp
from jax import lax
from jax.experimental import pallas as pl
from jax.experimental.pallas import tpu as pltpu
from jax.sharding import PartitionSpec as P

CAP = 36
SLOTS = -(-CAP // 8) * 8

f32 = jnp.float32
bf16 = jnp.bfloat16
VMEM_LIMIT = 56 * 1024 * 1024


def nt(a, b):
    return lax.dot_general(a, b, (((1,), (1,)), ((), ())), preferred_element_type=f32)


def nn(a, b):
    return lax.dot_general(a, b, (((1,), (0,)), ((), ())), preferred_element_type=f32)


def tn(a, b):
    return lax.dot_general(a, b, (((0,), (0,)), ((), ())), preferred_element_type=f32)


def shifted(value, axis, steps):
    count = lax.axis_size(axis)
    initial, last = (max(0, -steps), min(count, count - steps))
    return lax.ppermute(value, axis, [(source, source + steps) for source in range(initial, last)])


def slot_targets(experts):
    tokens = experts.shape[1]
    same = experts[:, :, :, None, None] == experts[:, None, None, :, :]
    earlier = jnp.arange(tokens)[:, None] > jnp.arange(tokens)[None, :]
    place = jnp.sum((same & earlier[None, :, None, :, None]).astype(jnp.int32), axis=(3, 4))
    return experts * SLOTS + place


def picks(rows, target):
    slot = lax.broadcasted_iota(jnp.int32, (rows, target.shape[-1]), 0)
    return slot == target[0:1], slot == target[1:2]


def fill(out_ref, one_hot, pieces_ref, first, tokens, gate=None):
    width = pieces_ref.shape[-1]
    for piece in range(pieces_ref.shape[0]):
        rows = nn(one_hot, pieces_ref[piece, first : first + tokens, :])
        if gate is not None:
            rows = rows * gate
        out_ref[:, piece * width : (piece + 1) * width] = rows.astype(bf16)


def step_dispatch_kernel(tokens, target_f, target_b, gates_b, pieces, x_ref, s_ref):
    first, second = picks(x_ref.shape[0], target_f[...])
    fill(x_ref, (first | second).astype(f32).astype(bf16), pieces, 0, tokens)
    first, second = picks(s_ref.shape[0], target_b[...])
    gate = jnp.sum(
        jnp.where(first, gates_b[0:1, :], 0.0) + jnp.where(second, gates_b[1:2, :], 0.0),
        axis=1,
        keepdims=True,
    )
    fill(s_ref, (first | second).astype(f32).astype(bf16), pieces, tokens, tokens, gate)


def saved_dispatch_kernel(tokens, target, pieces, *outs):
    for tick, out_ref in enumerate(outs):
        first, second = picks(out_ref.shape[0], target[tick])
        fill(out_ref, (first | second).astype(f32).astype(bf16), pieces, tick * tokens, tokens)


def combine_kernel(target_f, gates_f, target_b, r_f, r_b, base_f, base_b, out_f, out_b):
    tokens, slots = base_f.shape[0], r_f.shape[0]
    slot = lax.broadcasted_iota(jnp.int32, (tokens, slots), 1)
    total = base_f[...].astype(f32)
    for k in range(2):
        pick = (slot == target_f[:, k : k + 1]).astype(f32).astype(bf16)
        total += gates_f[:, k : k + 1] * nn(pick, r_f[...])
    out_f[...] = total.astype(bf16)
    pick = ((slot == target_b[:, 0:1]) | (slot == target_b[:, 1:2])).astype(f32).astype(bf16)
    out_b[...] = (base_b[...].astype(f32) + nn(pick, r_b[...])).astype(bf16)


def put_pieces(out_ref, acc_ref):
    width = out_ref.shape[-1]
    for piece in range(out_ref.shape[0]):
        out_ref[piece] = acc_ref[:, piece * width : (piece + 1) * width].astype(bf16)


def first_step_kernel(
    xf, xb0, xb1, s0, gate, down, out_f, out_b, hid, slope, tilt, xs, acc_f, acc_b
):
    rows = xf.shape[0]
    step = pl.program_id(0)

    @pl.when(step == 0)
    def _():
        xs[0:rows, :] = xf[...]
        xs[rows : 2 * rows, :] = xb0[...]
        xs[2 * rows : 3 * rows, :] = xb1[...]
        acc_f[...] = jnp.zeros_like(acc_f)
        acc_b[...] = jnp.zeros_like(acc_b)

    pre = nt(xs[...], gate[...])
    sig = 1.0 / (1.0 + jnp.exp(-pre))
    hidden = (pre * sig).astype(bf16)
    hid[...] = hidden[rows:]
    acc_f[...] += nn(hidden[:rows], down[...])
    bend = sig[rows:] * (1.0 + pre[rows:] * (1.0 - sig[rows:]))
    tilt[...] = bend[rows:]
    through = nt(s0[...], down[...])
    sl = (through * bend[:rows]).astype(bf16)
    slope[...] = sl
    acc_b[...] += nn(sl, gate[...])

    @pl.when(step == pl.num_programs(0) - 1)
    def _():
        put_pieces(out_f, acc_f)
        put_pieces(out_b, acc_b)


def second_step_kernel(
    xf, s1, s0, xb0, xb1, gate, down, hid, slope0, tilt, out_f, out_b, slope1, squares,
    acc_f, acc_b, gram_h, gram_l,
):
    rows = xf.shape[0]
    step = pl.program_id(0)

    @pl.when(step == 0)
    def _():
        acc_f[...] = jnp.zeros_like(acc_f)
        acc_b[...] = jnp.zeros_like(acc_b)
        gram_h[...] = jnp.zeros_like(gram_h)
        gram_l[...] = jnp.zeros_like(gram_l)

    pre = nt(xf[...], gate[...])
    hidden = (pre / (1.0 + jnp.exp(-pre))).astype(bf16)
    acc_f[...] += nn(hidden, down[...])
    through = nt(s1[...], down[...])
    sl = (through * tilt[...]).astype(bf16)
    slope1[...] = sl
    acc_b[...] += nn(sl, gate[...])
    both = hid[...]
    gram_h[...] += nt(both, both)
    slopes = jnp.concatenate([slope0[...], sl], axis=0)
    gram_l[...] += nt(slopes, slopes)

    @pl.when(step == pl.num_programs(0) - 1)
    def _():
        put_pieces(out_f, acc_f)
        put_pieces(out_b, acc_b)
        scaled = jnp.concatenate([s0[...], s1[...]], axis=0)
        stored = jnp.concatenate([xb0[...], xb1[...]], axis=0)
        total = jnp.sum(gram_h[...] * nt(scaled, scaled) + gram_l[...] * nt(stored, stored))
        squares[...] = jnp.full(squares.shape, total, f32)


def grad_kernel(factor, xb0, xb1, s0, s1, hid, slope0, slope1, gate_out, down_out):
    rows = xb0.shape[0]
    scale = factor[0]
    down_sum = tn(hid[0:rows, :], s0[...]) + tn(hid[rows : 2 * rows, :], s1[...])
    down_out[...] = (down_sum * scale).astype(bf16)
    gate_sum = tn(slope0[...], xb0[...]) + tn(slope1[...], xb1[...])
    gate_out[...] = (gate_sum * scale).astype(bf16)


def params():
    return pltpu.CompilerParams(
        dimension_semantics=("arbitrary",), vmem_limit_bytes=VMEM_LIMIT
    )


def plain(kernel, shapes, name):
    return pl.pallas_call(
        kernel,
        out_shape=[jax.ShapeDtypeStruct(s, bf16) for s in shapes],
        name=name,
        compiler_params=pltpu.CompilerParams(vmem_limit_bytes=VMEM_LIMIT),
    )


def whole_spec(array):
    return pl.BlockSpec(array.shape, lambda i: (0,) * len(array.shape))


def on_device(
    fwd_input,
    fresh_input,
    fwd_experts,
    fwd_gates,
    bwd_saved,
    bwd_experts,
    bwd_gates,
    out_grad,
    fresh_grad,
    gate_proj,
    down_proj,
):
    gate_weight = gate_proj[0, 0]
    down_weight = down_proj[0, 0]
    hidden_units, width = gate_weight.shape
    section_count = lax.axis_size("section")
    expert_count = lax.axis_size("dp")
    feature_parts = lax.axis_size("expert")
    section_index = lax.axis_index("section")
    is_first = section_index == 0
    is_last = section_index == section_count - 1
    tick_count, tokens = fwd_experts.shape[1], fwd_experts.shape[2]
    part = fwd_input.shape[-1]
    rows = expert_count * SLOTS
    block = 512 if hidden_units % 512 == 0 else hidden_units
    steps = hidden_units // block

    targets_f = slot_targets(fwd_experts[0])
    targets_b = slot_targets(bwd_experts[0])
    lanes_f = jnp.swapaxes(targets_f, 1, 2)
    lanes_b = jnp.swapaxes(targets_b, 1, 2)
    gate_lanes_b = jnp.swapaxes(bwd_gates[0], 1, 2)

    def over_dp(value):
        return lax.all_to_all(value, "dp", split_axis=0, concat_axis=0, tiled=True)

    def dispatch(tick, input_part, grad_part):
        pieces = lax.all_gather(jnp.concatenate([input_part, grad_part], axis=0), "expert", axis=0)
        x, s = plain(
            functools.partial(step_dispatch_kernel, tokens),
            [(rows, width)] * 2,
            "step_dispatch",
        )(lanes_f[tick], lanes_b[tick], gate_lanes_b[tick], pieces)
        return over_dp(x), over_dp(s)

    def collect(tick, partial_f, partial_b, input_part, grad_part):
        swapped = lax.all_to_all(
            jnp.concatenate([partial_f, partial_b], axis=1),
            "expert", split_axis=0, concat_axis=0, tiled=True,
        )
        summed = jnp.sum(swapped.astype(f32), axis=0).astype(bf16)
        r_f, r_b = over_dp(summed[:rows]), over_dp(summed[rows:])
        return plain(combine_kernel, [(tokens, part)] * 2, "combine")(
            targets_f[tick], fwd_gates[0, tick], targets_b[tick], r_f, r_b, input_part, grad_part
        )

    saved_pieces = lax.all_gather(bwd_saved[0].reshape(tick_count * tokens, part), "expert", axis=0)
    stored = plain(
        functools.partial(saved_dispatch_kernel, tokens),
        [(rows, width)] * tick_count,
        "saved_dispatch",
    )(lanes_b, saved_pieces)
    stored0, stored1 = [over_dp(value) for value in stored]

    input_part, grad_part = fwd_input[0], out_grad[0]
    x0, scaled0 = dispatch(0, input_part, grad_part)

    def unit_block(count):
        return pl.BlockSpec((count, block), lambda i: (0, i))

    weight_spec = pl.BlockSpec((block, width), lambda i: (i, 0))
    pieces_shape = jax.ShapeDtypeStruct((feature_parts, rows, part), bf16)
    pieces_spec = whole_spec(pieces_shape)
    row_spec = whole_spec(x0)
    matmul = 2 * rows * hidden_units * width
    weight_bytes = 4 * hidden_units * width
    out_f, out_b, hid, slope0, tilt = pl.pallas_call(
        first_step_kernel,
        grid=(steps,),
        in_specs=[row_spec] * 4 + [weight_spec] * 2,
        out_specs=[pieces_spec] * 2 + [unit_block(2 * rows), unit_block(rows), unit_block(rows)],
        out_shape=[
            pieces_shape,
            pieces_shape,
            jax.ShapeDtypeStruct((2 * rows, hidden_units), bf16),
            jax.ShapeDtypeStruct((rows, hidden_units), bf16),
            jax.ShapeDtypeStruct((rows, hidden_units), f32),
        ],
        scratch_shapes=[
            pltpu.VMEM((3 * rows, width), bf16),
            pltpu.VMEM((rows, width), f32),
            pltpu.VMEM((rows, width), f32),
        ],
        compiler_params=params(),
        cost_estimate=pl.CostEstimate(
            flops=6 * matmul, bytes_accessed=weight_bytes, transcendentals=0
        ),
        name="first_step",
    )(x0, stored0, stored1, scaled0, gate_weight, down_weight)
    produced0, returned0 = collect(0, out_f, out_b, input_part, grad_part)

    arriving = shifted(produced0, "section", 1)
    leaving = shifted(returned0, "section", -1)
    input_part = jnp.where(is_first, fresh_input[0], arriving)
    grad_part = jnp.where(is_last, fresh_grad[0], leaving)
    x1, scaled1 = dispatch(1, input_part, grad_part)
    out_f, out_b, slope1, squares = pl.pallas_call(
        second_step_kernel,
        grid=(steps,),
        in_specs=[row_spec] * 5
        + [weight_spec] * 2
        + [unit_block(2 * rows), unit_block(rows), unit_block(rows)],
        out_specs=[pieces_spec] * 2
        + [unit_block(rows), pl.BlockSpec((8, 128), lambda i: (0, 0))],
        out_shape=[
            pieces_shape,
            pieces_shape,
            jax.ShapeDtypeStruct((rows, hidden_units), bf16),
            jax.ShapeDtypeStruct((8, 128), f32),
        ],
        scratch_shapes=[
            pltpu.VMEM((rows, width), f32),
            pltpu.VMEM((rows, width), f32),
            pltpu.VMEM((2 * rows, 2 * rows), f32),
            pltpu.VMEM((2 * rows, 2 * rows), f32),
        ],
        compiler_params=params(),
        cost_estimate=pl.CostEstimate(
            flops=4 * matmul, bytes_accessed=weight_bytes, transcendentals=0
        ),
        name="second_step",
    )(x1, scaled1, scaled0, stored0, stored1, gate_weight, down_weight, hid, slope0, tilt)

    everyone = lax.all_gather(squares, ("section", "expert", "dp"), axis=0)
    total = jnp.sum(everyone[:, 0, 0])
    clip_limit = 0.25 * math.sqrt(
        2.0 * section_count * expert_count * feature_parts * hidden_units * width
    )
    factor = clip_limit / jnp.maximum(jnp.sqrt(total), clip_limit)
    produced1, returned1 = collect(1, out_f, out_b, input_part, grad_part)

    gate_grad, down_grad = pl.pallas_call(
        grad_kernel,
        grid=(steps,),
        in_specs=[pl.BlockSpec(memory_space=pltpu.SMEM)]
        + [row_spec] * 4
        + [unit_block(2 * rows), unit_block(rows), unit_block(rows)],
        out_specs=[weight_spec] * 2,
        out_shape=[jax.ShapeDtypeStruct((hidden_units, width), bf16)] * 2,
        compiler_params=params(),
        cost_estimate=pl.CostEstimate(
            flops=4 * matmul, bytes_accessed=weight_bytes, transcendentals=0
        ),
        name="weight_grads",
    )(factor.reshape(1), stored0, stored1, scaled0, scaled1, hid, slope0, slope1)

    fwd_output = jnp.stack([produced0, produced1])[None]
    input_grad = jnp.stack([returned0, returned1])[None]
    return (fwd_output, input_grad, gate_grad[None, None], down_grad[None, None])


def solution(mesh):
    in_specs = (
        P("section", "dp", "expert"),
        P(None, "dp", "expert"),
        P("section", None, "dp", None),
        P("section", None, "dp", None),
        P("section", None, "dp", "expert"),
        P("section", None, "dp", None),
        P("section", None, "dp", None),
        P("section", "dp", "expert"),
        P(None, "dp", "expert"),
        P("section", "dp", "expert", None),
        P("section", "dp", "expert", None),
    )
    out_specs = (
        P("section", None, "dp", "expert"),
        P("section", None, "dp", "expert"),
        P("section", "dp", "expert", None),
        P("section", "dp", "expert", None),
    )
    return jax.shard_map(
        on_device, mesh=mesh, in_specs=in_specs, out_specs=out_specs, check_vma=False
    )
```

```python
import functools
import math

import jax
import jax.numpy as jnp
from jax import lax
from jax.experimental import pallas as pl
from jax.experimental.pallas import tpu as pltpu
from jax.sharding import PartitionSpec as P

CAP = 36
SLOTS = -(-CAP // 8) * 8

f32 = jnp.float32
bf16 = jnp.bfloat16
VMEM_LIMIT = 56 * 1024 * 1024


def nt(a, b):
    return lax.dot_general(a, b, (((1,), (1,)), ((), ())), preferred_element_type=f32)


def nn(a, b):
    return lax.dot_general(a, b, (((1,), (0,)), ((), ())), preferred_element_type=f32)


def tn(a, b):
    return lax.dot_general(a, b, (((0,), (0,)), ((), ())), preferred_element_type=f32)


def slot_targets(experts):
    tokens = experts.shape[1]
    same = experts[:, :, :, None, None] == experts[:, None, None, :, :]
    earlier = jnp.arange(tokens)[:, None] > jnp.arange(tokens)[None, :]
    place = jnp.sum((same & earlier[None, :, None, :, None]).astype(jnp.int32), axis=(3, 4))
    return experts * SLOTS + place


def ring(axis, step):
    return lax.rem(lax.axis_index(axis) + step, lax.axis_size(axis))


def greet(places):
    barrier = pltpu.get_barrier_semaphore()
    for place in places:
        pl.semaphore_signal(
            barrier, inc=1, device_id=place, device_id_type=pl.DeviceIdType.MESH
        )
    pl.semaphore_wait(barrier, len(places))


def peers(axis):
    return [{axis: ring(axis, step)} for step in range(1, lax.axis_size(axis))]


def remote(source, target, send, recv, place):
    copy = pltpu.make_async_remote_copy(
        src_ref=source,
        dst_ref=target,
        send_sem=send,
        recv_sem=recv,
        device_id=place,
        device_id_type=pl.DeviceIdType.MESH,
    )
    copy.start()
    return copy


def wait_all(copies):
    for copy in copies:
        copy.wait()


def gather_pieces(source, pieces, send, recv):
    me = lax.axis_index("expert")
    copies = [
        remote(source, pieces.at[me], send.at[step], recv.at[step], place)
        for step, place in enumerate(peers("expert"))
    ]
    pieces[me] = source[...]
    return copies


def send_slots(out, buffer, pieces, target, gates, send, recv):
    count, slots = out.shape[0], out.shape[1]
    parts, tokens, part = pieces.shape
    me = lax.axis_index("dp")
    copies = []
    for step in [*range(1, count), 0]:
        home = ring("dp", step)
        slot = lax.broadcasted_iota(jnp.int32, (slots, tokens), 0) + home * slots
        first, second = slot == target[0:1], slot == target[1:2]
        one_hot = (first | second).astype(f32).astype(bf16)
        if gates is not None:
            gate = jnp.sum(
                jnp.where(first, gates[0:1], 0.0) + jnp.where(second, gates[1:2], 0.0),
                axis=1,
                keepdims=True,
            )
        for piece in range(parts):
            rows = nn(one_hot, pieces[piece])
            if gates is not None:
                rows = rows * gate
            columns = slice(piece * part, (piece + 1) * part)
            if step:
                buffer[step - 1, :, columns] = rows.astype(bf16)
            else:
                out[me, :, columns] = rows.astype(bf16)
        if step:
            copies.append(
                remote(
                    buffer.at[step - 1], out.at[me], send.at[step - 1], recv.at[step - 1],
                    {"dp": home},
                )
            )
    return copies


def start_partials(partials, arrived, send, recv):
    copies = {}
    count = partials[0].shape[1]
    for step in [*range(1, count), 0]:
        home = ring("dp", step)
        for stream, partial in enumerate(partials):
            copies[stream, step] = [
                remote(
                    partial.at[place["expert"], home],
                    arrived[stream].at[turn, step],
                    send.at[stream, turn, step],
                    recv.at[stream, turn, step],
                    place,
                )
                for turn, place in enumerate(peers("expert"))
            ]
    return copies


def finish_partials(copies, partials, arrived, buffers, returned, send, recv):
    parts, count = partials[0].shape[0], partials[0].shape[1]
    mine, me = lax.axis_index("expert"), lax.axis_index("dp")
    leaving = []
    for step in [*range(1, count), 0]:
        home = ring("dp", step)
        for stream, partial in enumerate(partials):
            wait_all(copies[stream, step])
            total = partial[mine, home].astype(f32)
            for turn in range(parts - 1):
                total += arrived[stream][turn, step].astype(f32)
            if step:
                buffers[stream][step - 1] = total.astype(bf16)
                leaving.append(
                    remote(
                        buffers[stream].at[step - 1],
                        returned[stream].at[me],
                        send.at[stream, step - 1],
                        recv.at[stream, step - 1],
                        {"dp": home},
                    )
                )
            else:
                returned[stream][me] = total.astype(bf16)
    return leaving


def combined(base, returned, target, gates):
    count, slots = returned.shape[0], returned.shape[1]
    tokens = base.shape[0]
    total = base.astype(f32)
    for number in range(count):
        slot = lax.broadcasted_iota(jnp.int32, (tokens, slots), 1) + number * slots
        for k in range(2):
            pick = (slot == target[:, k : k + 1]).astype(f32).astype(bf16)
            rows = nn(pick, returned[number])
            total += rows if gates is None else gates[:, k : k + 1] * rows
    return total.astype(bf16)


def enter_kernel(
    lanes_f, lanes_b, gate_lanes_b, fwd, grad, saved, x0, s0, *rest
):
    ticks = saved.shape[0]
    stored, (pieces, buffers, send_y, recv_y, send_z, recv_z) = rest[:ticks], rest[ticks:]
    greet(peers("expert") + peers("dp"))
    sources = [fwd, saved.at[0], grad] + [saved.at[tick] for tick in range(1, ticks)]
    outs = [x0, stored[0], s0] + list(stored[1:])
    targets = [lanes_f[0], lanes_b[0], lanes_b[0]] + [lanes_b[tick] for tick in range(1, ticks)]
    gates = [None, None, gate_lanes_b[0]] + [None] * (ticks - 1)
    gathers = [
        gather_pieces(source, pieces.at[i], send_y.at[i], recv_y.at[i])
        for i, source in enumerate(sources)
    ]
    leaving = []
    for i, out in enumerate(outs):
        wait_all(gathers[i])
        leaving += send_slots(
            out, buffers.at[i], pieces.at[i], targets[i], gates[i], send_z.at[i], recv_z.at[i]
        )
    wait_all(leaving)


def section_places(step):
    count = lax.axis_size("section")
    return [
        {"section": ring("section", step % count), "expert": ring("expert", turn)}
        for turn in range(lax.axis_size("expert"))
    ]


def turn_kernel(
    tick, targets_f, gates_f, targets_b, lanes_f, lanes_b, gate_lanes_b,
    partial_f, partial_b, base_f, base_b, fresh_f, fresh_b,
    out_f, out_b, next_f, next_b, x, s,
    arrived_f, arrived_b, buffer_f, buffer_b, returned_f, returned_b,
    fresh, fresh_pieces, pieces, slot_buffers,
    send_p, recv_p, send_r, recv_r, send_n, recv_n, send_x, recv_x, send_z, recv_z,
):
    section, mine = lax.axis_index("section"), lax.axis_index("expert")
    is_first, is_last = section == 0, section == lax.axis_size("section") - 1
    greet(peers("expert") + peers("dp") + section_places(1) + section_places(-1))
    partials, arrived = (partial_f, partial_b), (arrived_f, arrived_b)
    copies = start_partials(partials, arrived, send_p, recv_p)
    fresh[...] = jnp.where(is_first, fresh_f[...], fresh_b[...])
    fresh_copies = gather_pieces(fresh, fresh_pieces, send_n, recv_n)
    leaving = finish_partials(
        copies, partials, arrived, (buffer_f, buffer_b), (returned_f, returned_b), send_r, recv_r
    )
    wait_all(leaving)
    shifts = []
    for stream, (out, step) in enumerate(((out_f, 1), (out_b, -1))):
        if stream == 0:
            out[...] = combined(base_f[...], returned_f, targets_f[tick], gates_f[tick])
        else:
            out[...] = combined(base_b[...], returned_b, targets_b[tick], None)
        shifts.append(
            [
                remote(
                    out, pieces.at[stream, mine], send_x.at[stream, turn], recv_x.at[stream, turn],
                    place,
                )
                for turn, place in enumerate(section_places(step))
            ]
        )
    wait_all(fresh_copies)
    ends, nexts, outs = (is_first, is_last), (next_f, next_b), (x, s)
    targets = (lanes_f[tick + 1], lanes_b[tick + 1])
    gates = (None, gate_lanes_b[tick + 1])
    leaving = []
    for stream in range(2):
        wait_all(shifts[stream])
        for piece in range(fresh_pieces.shape[0]):
            pieces[stream, piece] = jnp.where(
                ends[stream], fresh_pieces[piece], pieces[stream, piece]
            )
        nexts[stream][...] = pieces[stream, mine]
        leaving += send_slots(
            outs[stream], slot_buffers.at[stream], pieces.at[stream], targets[stream],
            gates[stream], send_z.at[stream], recv_z.at[stream],
        )
    wait_all(leaving)


def leave_kernel(
    tick, targets_f, gates_f, targets_b, partial_f, partial_b, base_f, base_b, old_f, old_b,
    squares, out_f, out_b, total,
    arrived_f, arrived_b, buffer_f, buffer_b, returned_f, returned_b, sums, landed,
    send_p, recv_p, send_r, recv_r, send_q, recv_q,
):
    greet(peers("section") + peers("expert") + peers("dp"))
    partials, arrived = (partial_f, partial_b), (arrived_f, arrived_b)

    current, slot = squares, 0
    for stage, axis in enumerate(("section", "expert", "dp")):
        others = peers(axis)
        small = [
            remote(
                current, landed.at[slot + turn], send_q.at[slot + turn], recv_q.at[slot + turn],
                place,
            )
            for turn, place in enumerate(others)
        ]
        if stage == 0:
            copies = start_partials(partials, arrived, send_p, recv_p)
        wait_all(small)
        value = current[...]
        for turn in range(len(others)):
            value += landed[slot + turn]
        if stage < 2:
            sums[stage] = value
            current = sums.at[stage]
        else:
            total[...] = value
        slot += len(others)

    leaving = finish_partials(
        copies, partials, arrived, (buffer_f, buffer_b), (returned_f, returned_b), send_r, recv_r
    )
    wait_all(leaving)
    for earlier in range(tick):
        out_f[earlier] = old_f[...]
        out_b[earlier] = old_b[...]
    out_f[tick] = combined(base_f[...], returned_f, targets_f[tick], gates_f[tick])
    out_b[tick] = combined(base_b[...], returned_b, targets_b[tick], None)


def talk(kernel, number, shapes, scratch, name):
    return pl.pallas_call(
        kernel,
        out_shape=[jax.ShapeDtypeStruct(*shape) for shape in shapes],
        scratch_shapes=scratch,
        compiler_params=pltpu.CompilerParams(
            vmem_limit_bytes=VMEM_LIMIT, collective_id=number, has_side_effects=True
        ),
        name=name,
    )


def put_pieces(out_ref, acc_ref):
    width = out_ref.shape[-1]
    for piece in range(out_ref.shape[0]):
        out_ref[piece] = acc_ref[:, piece * width : (piece + 1) * width].astype(bf16)


def first_step_kernel(
    xf, xb0, xb1, s0, gate, down, out_f, out_b, hid, slope, tilt, xs, acc_f, acc_b
):
    rows = xf.shape[0]
    step = pl.program_id(0)

    @pl.when(step == 0)
    def _():
        xs[0:rows, :] = xf[...]
        xs[rows : 2 * rows, :] = xb0[...]
        xs[2 * rows : 3 * rows, :] = xb1[...]
        acc_f[...] = jnp.zeros_like(acc_f)
        acc_b[...] = jnp.zeros_like(acc_b)

    pre = nt(xs[...], gate[...])
    sig = 1.0 / (1.0 + jnp.exp(-pre))
    hidden = (pre * sig).astype(bf16)
    hid[...] = hidden[rows:]
    acc_f[...] += nn(hidden[:rows], down[...])
    bend = sig[rows:] * (1.0 + pre[rows:] * (1.0 - sig[rows:]))
    tilt[...] = bend[rows:]
    through = nt(s0[...], down[...])
    sl = (through * bend[:rows]).astype(bf16)
    slope[...] = sl
    acc_b[...] += nn(sl, gate[...])

    @pl.when(step == pl.num_programs(0) - 1)
    def _():
        put_pieces(out_f, acc_f)
        put_pieces(out_b, acc_b)


def second_step_kernel(
    xf, s1, s0, xb0, xb1, gate, down, hid, slope0, tilt, out_f, out_b, slope1, squares,
    acc_f, acc_b, gram_h, gram_l,
):
    rows = xf.shape[0]
    step = pl.program_id(0)

    @pl.when(step == 0)
    def _():
        acc_f[...] = jnp.zeros_like(acc_f)
        acc_b[...] = jnp.zeros_like(acc_b)
        gram_h[...] = jnp.zeros_like(gram_h)
        gram_l[...] = jnp.zeros_like(gram_l)

    pre = nt(xf[...], gate[...])
    hidden = (pre / (1.0 + jnp.exp(-pre))).astype(bf16)
    acc_f[...] += nn(hidden, down[...])
    through = nt(s1[...], down[...])
    sl = (through * tilt[...]).astype(bf16)
    slope1[...] = sl
    acc_b[...] += nn(sl, gate[...])
    both = hid[...]
    gram_h[...] += nt(both, both)
    slopes = jnp.concatenate([slope0[...], sl], axis=0)
    gram_l[...] += nt(slopes, slopes)

    @pl.when(step == pl.num_programs(0) - 1)
    def _():
        put_pieces(out_f, acc_f)
        put_pieces(out_b, acc_b)
        scaled = jnp.concatenate([s0[...], s1[...]], axis=0)
        stored = jnp.concatenate([xb0[...], xb1[...]], axis=0)
        total = jnp.sum(gram_h[...] * nt(scaled, scaled) + gram_l[...] * nt(stored, stored))
        squares[...] = jnp.full(squares.shape, total, f32)


def grad_kernel(clip_limit, squares, xb0, xb1, s0, s1, hid, slope0, slope1, gate_out, down_out):
    rows = xb0.shape[0]
    norm = jnp.sqrt(squares[0:1, 0:1])
    scale = clip_limit / jnp.maximum(norm, clip_limit)
    down_sum = tn(hid[0:rows, :], s0[...]) + tn(hid[rows : 2 * rows, :], s1[...])
    down_out[...] = (down_sum * scale).astype(bf16)
    gate_sum = tn(slope0[...], xb0[...]) + tn(slope1[...], xb1[...])
    gate_out[...] = (gate_sum * scale).astype(bf16)


def params():
    return pltpu.CompilerParams(
        dimension_semantics=("arbitrary",), vmem_limit_bytes=VMEM_LIMIT
    )


def whole_spec(array):
    return pl.BlockSpec(array.shape, lambda i: (0,) * len(array.shape))


def on_device(
    fwd_input,
    fresh_input,
    fwd_experts,
    fwd_gates,
    bwd_saved,
    bwd_experts,
    bwd_gates,
    out_grad,
    fresh_grad,
    gate_proj,
    down_proj,
):
    gate_weight = gate_proj[0, 0]
    down_weight = down_proj[0, 0]
    hidden_units, width = gate_weight.shape
    section_count = lax.axis_size("section")
    expert_count = lax.axis_size("dp")
    feature_parts = lax.axis_size("expert")
    tick_count, tokens = fwd_experts.shape[1], fwd_experts.shape[2]
    part = fwd_input.shape[-1]
    rows = expert_count * SLOTS
    block = 512 if hidden_units % 512 == 0 else hidden_units
    steps = hidden_units // block

    targets_f = slot_targets(fwd_experts[0])
    targets_b = slot_targets(bwd_experts[0])
    lanes_f = jnp.swapaxes(targets_f, 1, 2)
    lanes_b = jnp.swapaxes(targets_b, 1, 2)
    gate_lanes_b = jnp.swapaxes(bwd_gates[0], 1, 2)

    dma = pltpu.SemaphoreType.DMA
    others, far = feature_parts - 1, expert_count - 1
    slot_shape = ((expert_count, SLOTS, width), bf16)
    part_shape = ((tokens, part), bf16)

    def flat(value):
        return value.reshape(rows, width)

    def split(value):
        return value.reshape(feature_parts, expert_count, SLOTS, part)

    def collect_scratch():
        return [
            *[pltpu.VMEM((others, expert_count, SLOTS, part), bf16)] * 2,
            *[pltpu.VMEM((far, SLOTS, part), bf16)] * 2,
            *[pltpu.VMEM((expert_count, SLOTS, part), bf16)] * 2,
        ]

    collect_sems = [
        *[dma((2, others, expert_count))] * 2,
        *[dma((2, far))] * 2,
    ]
    streams = 2 + tick_count
    input_part, grad_part = fwd_input[0], out_grad[0]
    x0, scaled0, stored0, stored1 = map(
        flat,
        talk(
            enter_kernel,
            0,
            [slot_shape] * streams,
            [
                pltpu.VMEM((streams, feature_parts, tokens, part), bf16),
                pltpu.VMEM((streams, far, SLOTS, width), bf16),
                *[dma((streams, others))] * 2,
                *[dma((streams, far))] * 2,
            ],
            "enter",
        )(lanes_f, lanes_b, gate_lanes_b, input_part, grad_part, bwd_saved[0]),
    )

    def unit_block(count):
        return pl.BlockSpec((count, block), lambda i: (0, i))

    weight_spec = pl.BlockSpec((block, width), lambda i: (i, 0))
    pieces_shape = jax.ShapeDtypeStruct((feature_parts, rows, part), bf16)
    pieces_spec = whole_spec(pieces_shape)
    row_spec = whole_spec(x0)
    matmul = 2 * rows * hidden_units * width
    weight_bytes = 4 * hidden_units * width
    out_f, out_b, hid, slope0, tilt = pl.pallas_call(
        first_step_kernel,
        grid=(steps,),
        in_specs=[row_spec] * 4 + [weight_spec] * 2,
        out_specs=[pieces_spec] * 2 + [unit_block(2 * rows), unit_block(rows), unit_block(rows)],
        out_shape=[
            pieces_shape,
            pieces_shape,
            jax.ShapeDtypeStruct((2 * rows, hidden_units), bf16),
            jax.ShapeDtypeStruct((rows, hidden_units), bf16),
            jax.ShapeDtypeStruct((rows, hidden_units), f32),
        ],
        scratch_shapes=[
            pltpu.VMEM((3 * rows, width), bf16),
            pltpu.VMEM((rows, width), f32),
            pltpu.VMEM((rows, width), f32),
        ],
        compiler_params=params(),
        cost_estimate=pl.CostEstimate(
            flops=6 * matmul, bytes_accessed=weight_bytes, transcendentals=0
        ),
        name="first_step",
    )(x0, stored0, stored1, scaled0, gate_weight, down_weight)
    produced0, returned0, input_part, grad_part, x1, scaled1 = talk(
        functools.partial(turn_kernel, 0),
        1,
        [part_shape] * 4 + [slot_shape] * 2,
        [
            *collect_scratch(),
            pltpu.VMEM((tokens, part), bf16),
            pltpu.VMEM((feature_parts, tokens, part), bf16),
            pltpu.VMEM((2, feature_parts, tokens, part), bf16),
            pltpu.VMEM((2, far, SLOTS, width), bf16),
            *collect_sems,
            *[dma((others,))] * 2,
            *[dma((2, feature_parts))] * 2,
            *[dma((2, far))] * 2,
        ],
        "turn",
    )(
        targets_f, fwd_gates[0], targets_b, lanes_f, lanes_b, gate_lanes_b,
        split(out_f), split(out_b), input_part, grad_part, fresh_input[0], fresh_grad[0],
    )
    x1, scaled1 = flat(x1), flat(scaled1)
    out_f, out_b, slope1, squares = pl.pallas_call(
        second_step_kernel,
        grid=(steps,),
        in_specs=[row_spec] * 5
        + [weight_spec] * 2
        + [unit_block(2 * rows), unit_block(rows), unit_block(rows)],
        out_specs=[pieces_spec] * 2
        + [unit_block(rows), pl.BlockSpec((8, 128), lambda i: (0, 0))],
        out_shape=[
            pieces_shape,
            pieces_shape,
            jax.ShapeDtypeStruct((rows, hidden_units), bf16),
            jax.ShapeDtypeStruct((8, 128), f32),
        ],
        scratch_shapes=[
            pltpu.VMEM((rows, width), f32),
            pltpu.VMEM((rows, width), f32),
            pltpu.VMEM((2 * rows, 2 * rows), f32),
            pltpu.VMEM((2 * rows, 2 * rows), f32),
        ],
        compiler_params=params(),
        cost_estimate=pl.CostEstimate(
            flops=4 * matmul, bytes_accessed=weight_bytes, transcendentals=0
        ),
        name="second_step",
    )(x1, scaled1, scaled0, stored0, stored1, gate_weight, down_weight, hid, slope0, tilt)

    clip_limit = 0.25 * math.sqrt(
        2.0 * section_count * expert_count * feature_parts * hidden_units * width
    )
    small = section_count - 1 + others + far
    result_shape = ((tick_count, tokens, part), bf16)
    fwd_output, input_grad, total = talk(
        functools.partial(leave_kernel, 1),
        2,
        [result_shape, result_shape, ((8, 128), f32)],
        [
            *collect_scratch(),
            pltpu.VMEM((2, 8, 128), f32),
            pltpu.VMEM((small, 8, 128), f32),
            *collect_sems,
            *[dma((small,))] * 2,
        ],
        "leave",
    )(
        targets_f, fwd_gates[0], targets_b, split(out_f), split(out_b), input_part, grad_part,
        produced0, returned0, squares,
    )

    gate_grad, down_grad = pl.pallas_call(
        functools.partial(grad_kernel, clip_limit),
        grid=(steps,),
        in_specs=[whole_spec(total)]
        + [row_spec] * 4
        + [unit_block(2 * rows), unit_block(rows), unit_block(rows)],
        out_specs=[weight_spec] * 2,
        out_shape=[jax.ShapeDtypeStruct((hidden_units, width), bf16)] * 2,
        compiler_params=params(),
        cost_estimate=pl.CostEstimate(
            flops=4 * matmul, bytes_accessed=weight_bytes, transcendentals=0
        ),
        name="weight_grads",
    )(total, stored0, stored1, scaled0, scaled1, hid, slope0, slope1)

    return (fwd_output[None], input_grad[None], gate_grad[None, None], down_grad[None, None])


def solution(mesh):
    in_specs = (
        P("section", "dp", "expert"),
        P(None, "dp", "expert"),
        P("section", None, "dp", None),
        P("section", None, "dp", None),
        P("section", None, "dp", "expert"),
        P("section", None, "dp", None),
        P("section", None, "dp", None),
        P("section", "dp", "expert"),
        P(None, "dp", "expert"),
        P("section", "dp", "expert", None),
        P("section", "dp", "expert", None),
    )
    out_specs = (
        P("section", None, "dp", "expert"),
        P("section", None, "dp", "expert"),
        P("section", "dp", "expert", None),
        P("section", "dp", "expert", None),
    )
    return jax.shard_map(
        on_device, mesh=mesh, in_specs=in_specs, out_specs=out_specs, check_vma=False
    )
```
